16 devices in a mesh: dp: 2 (over y, z), tp: 8 (over x, core).
Axes of the slice: x: 4, y: 2, z: 1, core: 2. Of those that a mesh axis runs over, the one named last changes fastest.
The devices are a block of a 4x4x8 slice.
Arguments:
- ids: int32 [32, 256], P('dp'), parts along dimension 0
- E: bfloat16 [16384, 3072], P('tp')
- g: bfloat16 [3072], replicated
- W: bfloat16 [3072, 12288], P(None, 'tp')
- du: bfloat16 [32, 256, 12288], P('dp', None, 'tp'), parts along dimension 0
- dres: bfloat16 [32, 256, 3072], P('dp', 'tp'), parts along dimension 0
Outputs:
- output 1: bfloat16 [32, 256, 12288], P('dp', None, 'tp'), parts along dimension 0
- output 2: bfloat16 [32, 256, 3072], P('dp', 'tp'), parts along dimension 0
- output 3: float32 [32768, 3072], P(('dp', 'tp')), parts along dimension 0
- output 4: float32 [6144, 12288], P('dp', 'tp'), parts along dimension 0
- output 5: float32 [6144], P('dp'), parts along dimension 0
There are 2 independent parts. The reference program is written for one: setup_inputs(seed, part) draws one part's arguments, and reference() takes and returns one part's arrays. A program takes and returns all parts, laid end to end along the dimension named above; an argument that names none is the same for every part.
All inputs are finite; a program needn't handle non-finite values.
Results may differ from the reference program's by a relative error of at most 0.001.
Values are sent between devices in bfloat16 or wider.
A program may use at most 768 MiB of HBM per device.

```python
import jax
import jax.numpy as jnp
from jax import lax

V = 16384
K = 16
T = 256
D = 3072
FC = 12288
TP = 8
NPOP = 256
EPS = 1e-6


def setup_inputs(seed: int = 0, part: int = 0) -> dict:
    key = jax.random.key(seed)
    kp = jax.random.fold_in(key, part)
    k1, k2, k3, k4, k5, k6 = jax.random.split(kp, 6)
    s1, s2, s3 = jax.random.split(key, 3)
    kd = jax.random.fold_in(kp, 7)
    d1, d2, d3, d4 = jax.random.split(kd, 4)
    vs = V // TP
    pop = jnp.arange(TP, dtype=jnp.int32) * vs + jax.random.randint(d1, (TP,), 0, vs, dtype=jnp.int32)
    pick = jax.random.randint(d2, (K, T), 0, TP, dtype=jnp.int32)
    uni = jax.random.randint(d3, (K, T), 0, V, dtype=jnp.int32)
    coin = jax.random.bernoulli(d4, 0.75, (K, T))
    ids = jnp.where(coin, pop[pick], uni).astype(jnp.int32)
    E = jax.random.normal(s1, (V, D), jnp.float32).astype(jnp.bfloat16)
    g = (1.0 + 0.4 * jax.random.normal(s2, (D,), jnp.float32)).astype(jnp.bfloat16)
    W = (jax.random.normal(s3, (D, FC), jnp.float32) * D ** -0.5).astype(jnp.bfloat16)
    du = jax.random.normal(k5, (K, T, FC), jnp.float32).astype(jnp.bfloat16)
    dres = jax.random.normal(k6, (K, T, D), jnp.float32).astype(jnp.bfloat16)
    return {"ids": ids, "E": E, "g": g, "W": W, "du": du, "dres": dres}


def reference(ids, E, g, W, du, dres):
    gf = g.astype(jnp.float32)
    fs = FC // TP
    wr = W.reshape(D, TP, fs).transpose(1, 0, 2)

    def micro(carry, inp):
        dE, dW, dg = carry
        idk, duk, dresk = inp
        x = jnp.take(E, idk, axis=0)
        xf = x.astype(jnp.float32)
        rs = lax.rsqrt(jnp.mean(xf * xf, axis=-1, keepdims=True) + EPS)
        nh = xf * rs
        n = (nh * gf).astype(jnp.bfloat16)
        u = jnp.dot(n, W, preferred_element_type=jnp.float32).astype(jnp.bfloat16)
        dur = duk.reshape(T, TP, fs).transpose(1, 0, 2)

        def add_block(acc, blk):
            dub, wb = blk
            pr = jnp.dot(dub, wb.T, preferred_element_type=jnp.float32)
            return acc + pr.astype(jnp.bfloat16).astype(jnp.float32), None

        dn, _ = lax.scan(add_block, jnp.zeros((T, D), jnp.float32), (dur, wr))
        gdn = gf * dn
        dx = dresk.astype(jnp.float32) + rs * (gdn - nh * jnp.mean(nh * gdn, axis=-1, keepdims=True))
        dxb = dx.astype(jnp.bfloat16).astype(jnp.float32)
        dE = dE.at[idk].add(dxb)
        dW = dW + jnp.dot(n.T, duk, preferred_element_type=jnp.float32)
        dg = dg + jnp.sum(dn * nh, axis=0)
        return (dE, dW, dg), (u, x)

    init = (jnp.zeros((V, D), jnp.float32), jnp.zeros((D, FC), jnp.float32), jnp.zeros((D,), jnp.float32))
    (dE, dW, dg), (u, x) = lax.scan(micro, init, (ids, du, dres))
    return u, x, dE, dW, dg
```

```python
import jax
import jax.numpy as jnp
from jax import lax
from jax.sharding import PartitionSpec as P

EPS = 1e-6
ROWS = 192
CAP = 96
CHUNKS = 4
HALF = CHUNKS // 2
LANES = 128


def solution(mesh):
    ntp = mesh.shape["tp"]
    nch = ntp // 2
    f32, bf16, i32 = jnp.float32, jnp.bfloat16, jnp.int32
    c0 = (((0,), (0,)), ((), ()))
    c1 = (((1,), (1,)), ((), ()))
    right = [(i, (i + 2) % ntp) for i in range(ntp)]
    left = [(i, (i - 2) % ntp) for i in range(ntp)]
    twin = [(i, i ^ 1) for i in range(ntp)]

    def dot(a, b, dims=(((1,), (0,)), ((), ()))):
        return lax.dot_general(a, b, dims, preferred_element_type=f32)

    def body(ids, E, g, W, du, dres):
        vs, d = E.shape
        nk, t = ids.shape
        ts = t // ntp
        fs = W.shape[1]
        nt = nk * t
        nl = nk * ts
        me = lax.axis_index("tp")
        ch, co = me // 2, me % 2
        lo = me * vs
        gf = g.astype(f32)

        kc = nk // CHUNKS
        ka = kc // 2

        def pick(a, chip, core, k0, k1):
            return lax.dynamic_slice(a, (k0, chip % nch, core, 0, 0), (k1 - k0, 1, 1, ts, d)).reshape(k1 - k0, ts, d).astype(f32)

        def pick1(a, chip, k0, k1):
            return lax.dynamic_slice(a, (k0, chip % nch, 0, 0), (k1 - k0, 1, ts, d)).reshape(k1 - k0, ts, d).astype(f32)

        ps, gots = [], []
        for c in range(CHUNKS):
            a = du[c * kc:(c + 1) * kc].reshape(kc * t, fs)
            p = dot(a, W, c1).astype(bf16).reshape(kc, nch, 2, ts, d)
            other = lax.dynamic_slice(p, (0, 0, 1 - co, 0, 0), (kc, nch, 1, ts, d)).reshape(kc, nch, ts, d)
            ps.append(p)
            gots.append(lax.ppermute(other, "tp", twin))

        def term(c, chip, k0, k1):
            return pick(ps[c], chip, co, k0, k1) + pick1(gots[c], chip, k0, k1)

        far, near = [], []
        for c in range(CHUNKS):
            ta, tb = term(c, ch + 2, 0, ka), term(c, ch + 2, ka, kc)
            far.append((lax.ppermute(ta, "tp", right), lax.ppermute(tb, "tp", left)))
            tr, tl = term(c, ch + 1, ka, kc), term(c, ch + nch - 1, 0, ka)
            near.append((lax.ppermute(tr, "tp", right), lax.ppermute(tl, "tp", left)))
        idf = ids.reshape(-1)
        nhi = ntp * vs // LANES
        per = vs // LANES
        ohi = (idf[:, None] // LANES == lax.broadcasted_iota(i32, (nt, nhi), 1)).astype(bf16)
        olo = (idf[:, None] % LANES == lax.broadcasted_iota(i32, (nt, LANES), 1)).astype(bf16)
        pres = (dot(ohi, olo, c0) > 0).astype(bf16)
        r0 = lax.broadcasted_iota(i32, (LANES, LANES), 0)
        r1 = lax.broadcasted_iota(i32, (LANES, LANES), 1)
        within = dot(pres, (r0 < r1).astype(bf16))
        h0 = lax.broadcasted_iota(i32, (nhi, nhi), 0)
        h1 = lax.broadcasted_iota(i32, (nhi, nhi), 1)
        above = dot(((h1 < h0) & (h0 // per == h1 // per)).astype(bf16), jnp.sum(pres.astype(f32), axis=1, keepdims=True).astype(bf16))
        smap = (within + above).astype(i32)
        s_hi, s_lo = (smap // LANES).astype(bf16), (smap % LANES).astype(bf16)
        slot = jnp.sum((dot(ohi, s_hi) * LANES + dot(ohi, s_lo)) * olo.astype(f32), axis=1).astype(i32)
        own = idf // vs
        idh = ids.reshape(nk, ntp, ts).transpose(1, 0, 2).reshape(ntp, nl)
        ownh = idh // vs
        oc = (ownh[:, None, :] == lax.broadcasted_iota(i32, (ntp, ntp, nl), 1)).astype(bf16).reshape(ntp * ntp, nl)
        j0 = lax.broadcasted_iota(i32, (nl, nl), 0)
        j1 = lax.broadcasted_iota(i32, (nl, nl), 1)
        before = dot(oc, (j0 < j1).astype(bf16))
        rank = jnp.sum((before * oc.astype(f32)).reshape(ntp, ntp, nl), axis=1).astype(i32)

        rmax = jnp.stack([jnp.max(slot) // ROWS, jnp.max(rank) // CAP]) + 1
        step = 1
        while step < mesh.shape["dp"]:
            ring = [(i, (i + step) % mesh.shape["dp"]) for i in range(mesh.shape["dp"])]
            rmax = jnp.maximum(rmax, lax.ppermute(rmax, "dp", ring))
            step *= 2
        rounds, xrounds = rmax[0], rmax[1]

        sm_me = lax.dynamic_slice_in_dim(jnp.where(pres > 0, smap, -1), me * per, per, 0).reshape(vs)

        def gather_round(r):
            oh = (lax.broadcasted_iota(i32, (ROWS, vs), 0) == (sm_me - r * ROWS)[None, :]).astype(bf16)
            xt = lax.all_gather(dot(oh, E).astype(bf16), "tp", axis=0, tiled=True)
            xf = xt.astype(f32)
            rs = lax.rsqrt(jnp.mean(xf * xf, axis=-1, keepdims=True) + EPS)
            ntab = ((xf * rs) * gf).astype(bf16)
            key = slot - r * ROWS
            tix = jnp.where((key >= 0) & (key < ROWS), own * ROWS + key, -1)
            oht = (tix[:, None] == lax.broadcasted_iota(i32, (nt, ntp * ROWS), 1)).astype(bf16)
            n = dot(oht, ntab).astype(bf16)
            tih = lax.dynamic_slice_in_dim(tix.reshape(nk, t), me * ts, ts, 1).reshape(-1)
            ohh = (tih[:, None] == lax.broadcasted_iota(i32, (nl, ntp * ROWS), 1)).astype(bf16)
            return n, dot(ohh, xt).astype(bf16)

        def more(c):
            r, n, xl = c
            n2, xl2 = gather_round(r)
            return r + 1, n + n2, xl + xl2

        n, xl = gather_round(0)
        _, n, xl = lax.while_loop(lambda c: c[0] < rounds, more, (i32(1), n, xl))

        relay = []

        def pass_on(c, chip):
            qa, qb = term(c, chip + 1, 0, ka) + far[c][0], term(c, chip + nch - 1, ka, kc) + far[c][1]
            relay.append((lax.ppermute(qa, "tp", right), lax.ppermute(qb, "tp", left)))

        chn, _ = lax.optimization_barrier((ch, n))
        for c in range(HALF):
            pass_on(c, chn)
        u = dot(n, W).astype(bf16)
        chu, _ = lax.optimization_barrier((ch, u))
        for c in range(HALF, CHUNKS):
            pass_on(c, chu)
        dns = []
        for c in range(CHUNKS):
            dns.append(term(c, chu, 0, ka) + relay[c][0] + near[c][1])
            dns.append(term(c, chu, ka, kc) + near[c][0] + relay[c][1])
        dn = jnp.concatenate(dns, axis=0).reshape(nl, d)

        xf = xl.astype(f32)
        rs = lax.rsqrt(jnp.mean(xf * xf, axis=-1, keepdims=True) + EPS)
        nh = xf * rs
        gdn = gf * dn
        dx = dres.reshape(nl, d).astype(f32) + rs * (gdn - nh * jnp.mean(nh * gdn, axis=-1, keepdims=True))
        dxb = dx.astype(bf16)
        dgp = jnp.sum(dn * nh, axis=0)
        dg = jnp.sum(lax.all_to_all(jnp.broadcast_to(dgp, (ntp, d)), "tp", 0, 0, tiled=True), axis=0)

        ownm = lax.dynamic_index_in_dim(ownh, me, 0, keepdims=False)
        rankm = lax.dynamic_index_in_dim(rank, me, 0, keepdims=False)

        def send_round(r):
            key = rankm - r * CAP
            q = jnp.where((key >= 0) & (key < CAP), ownm * CAP + key, -1)
            oh = (lax.broadcasted_iota(i32, (ntp * CAP, nl), 0) == q[None, :]).astype(bf16)
            b = dot(oh, dxb).astype(bf16)
            got = lax.all_to_all(b.reshape(ntp, CAP, d), "tp", 0, 0, tiled=True).reshape(ntp * CAP, d)
            hit = (ownh == me)[:, None, :] & ((rank - r * CAP)[:, None, :] == lax.broadcasted_iota(i32, (ntp, CAP, nl), 1))
            rows = (jnp.sum(jnp.where(hit, (idh - lo + 1)[:, None, :], 0), axis=2) - 1).reshape(-1)
            ohr = (lax.broadcasted_iota(i32, (vs, ntp * CAP), 0) == rows[None, :]).astype(bf16)
            return dot(ohr, got)

        dE = send_round(0)
        dW = dot(n, du.reshape(nt, fs), c0)
        _, dE = lax.while_loop(lambda c: c[0] < xrounds, lambda c: (c[0] + 1, c[1] + send_round(c[0])), (i32(1), dE))
        return u.reshape(nk, t, fs), xl.reshape(nk, ts, d), dE, dW, dg

    return jax.shard_map(
        body,
        mesh=mesh,
        in_specs=(P("dp", None), P("tp", None), P(None), P(None, "tp"), P("dp", None, "tp"), P("dp", "tp", None)),
        out_specs=(P("dp", None, "tp"), P("dp", "tp", None), P(("dp", "tp"), None), P("dp", "tp"), P("dp")),
        check_vma=False,
    )
```

```python
import jax
import jax.numpy as jnp
from jax import lax
from jax.sharding import PartitionSpec as P


EPS = 1e-6
ROWS = 176
CAP = 96
LANES = 128


def solution(mesh):
    ntp = mesh.shape["tp"]
    nch = ntp // 2
    f32, bf16, i32 = jnp.float32, jnp.bfloat16, jnp.int32
    c0 = (((0,), (0,)), ((), ()))
    c1 = (((1,), (1,)), ((), ()))
    right = [(i, (i + 2) % ntp) for i in range(ntp)]
    left = [(i, (i - 2) % ntp) for i in range(ntp)]
    twin = [(i, i ^ 1) for i in range(ntp)]

    def dot(a, b, dims=(((1,), (0,)), ((), ()))):
        return lax.dot_general(a, b, dims, preferred_element_type=f32)

    def send(a, ring, axis="tp"):
        return lax.ppermute(a, axis, ring)

    def mm(*a):
        return dot(*a).astype(bf16)

    def tie(a, b):
        return lax.optimization_barrier((a, b))[0]

    def work(ids, E, g, W, du, dres):
        vs, d = E.shape
        nk, t = ids.shape
        ts = t // ntp
        fs = W.shape[1]
        nt = nk * t
        nl = nk * ts
        me = lax.axis_index("tp")
        ch, co = me // 2, me % 2
        lo = me * vs
        gf = g.astype(f32)

        sizes = (nk // 4, nk // 2, nk // 4)
        starts = (0, nk // 4, 3 * nk // 4)
        nc = len(sizes)

        def pick(a, chip, core, k0, k1):
            return lax.dynamic_slice(a, (k0, chip % nch, core, 0, 0), (k1 - k0, 1, 1, ts, d)).reshape(k1 - k0, ts, d).astype(f32)

        def pick1(a, chip, k0, k1):
            return lax.dynamic_slice(a, (k0, chip % nch, 0, 0), (k1 - k0, 1, ts, d)).reshape(k1 - k0, ts, d).astype(f32)

        ps, gots, near = [], [], []

        def term(c, chip, k0, k1):
            return pick(ps[c], chip, co, k0, k1) + pick1(gots[c], chip, k0, k1)

        def after(c, x):
            ps[c], gots[c], _ = lax.optimization_barrier((ps[c], gots[c], x))

        def spread(c):
            kc, ka = sizes[c], sizes[c] // 2
            to_r = jnp.concatenate([term(c, ch + 2, 0, ka), term(c, ch + 1, ka, kc)], axis=0)
            to_l = jnp.concatenate([term(c, ch + nch - 1, 0, ka), term(c, ch + 2, ka, kc)], axis=0)
            to_r, to_l = lax.optimization_barrier((to_r, to_l))
            near.append((send(to_r, right), send(to_l, left)))
            return to_l

        for c in range(nc):
            kc = sizes[c]
            a = du[starts[c]:starts[c] + kc].reshape(kc * t, fs)
            p = mm(a, W, c1).reshape(kc, nch, 2, ts, d)
            other = lax.dynamic_slice(p, (0, 0, 1 - co, 0, 0), (kc, nch, 1, ts, d)).reshape(kc, nch, ts, d)
            ps.append(p)
            gots.append(send(other, twin))
        for c in range(nc):
            last = spread(c)

        relay = []

        def pass_on(c, chip):
            kc, ka = sizes[c], sizes[c] // 2
            qa = term(c, chip + 1, 0, ka) + near[c][0][:ka]
            qb = term(c, chip + nch - 1, ka, kc) + near[c][1][ka:]
            relay.append((send(qa, right), send(qb, left)))

        after(0, last)
        pass_on(0, ch)

        idf = ids.reshape(-1)
        nhi = ntp * vs // LANES
        per = vs // LANES
        ohi = (idf[:, None] // LANES == lax.broadcasted_iota(i32, (nt, nhi), 1)).astype(bf16)
        olo = (idf[:, None] % LANES == lax.broadcasted_iota(i32, (nt, LANES), 1)).astype(bf16)
        pres = (dot(ohi, olo, c0) > 0).astype(bf16)
        r0 = lax.broadcasted_iota(i32, (LANES, LANES), 0)
        r1 = lax.broadcasted_iota(i32, (LANES, LANES), 1)
        within = dot(pres, (r0 < r1).astype(bf16))
        h0 = lax.broadcasted_iota(i32, (nhi, nhi), 0)
        h1 = lax.broadcasted_iota(i32, (nhi, nhi), 1)
        above = dot(((h1 < h0) & (h0 // per == h1 // per)).astype(bf16), jnp.sum(pres.astype(f32), axis=1, keepdims=True).astype(bf16))
        smap = (within + above).astype(i32)
        s_hi, s_lo = (smap // LANES).astype(bf16), (smap % LANES).astype(bf16)
        slot = jnp.sum((dot(ohi, s_hi) * LANES + dot(ohi, s_lo)) * olo.astype(f32), axis=1).astype(i32)
        own = idf // vs
        away = (own // 2 + nch - ch) % nch
        place = jnp.where(own % 2 == co, 0, nch) + jnp.where(away == 0, 0, jnp.where(away == nch - 1, 1, away + 1))
        idh = ids.reshape(nk, ntp, ts).transpose(1, 0, 2).reshape(ntp, nl)
        ownh = idh // vs
        oc = (ownh[:, None, :] == lax.broadcasted_iota(i32, (ntp, ntp, nl), 1)).astype(bf16).reshape(ntp * ntp, nl)
        j0 = lax.broadcasted_iota(i32, (nl, nl), 0)
        j1 = lax.broadcasted_iota(i32, (nl, nl), 1)
        before = dot(oc, (j0 < j1).astype(bf16))
        rank = jnp.sum((before * oc.astype(f32)).reshape(ntp, ntp, nl), axis=1).astype(i32)

        rmax = jnp.stack([jnp.max(slot) // ROWS, jnp.max(rank) // CAP]) + 1
        step = 1
        while step < mesh.shape["dp"]:
            ring = [(i, (i + step) % mesh.shape["dp"]) for i in range(mesh.shape["dp"])]
            rmax = jnp.maximum(rmax, send(rmax, ring, "dp"))
            step *= 2
        rounds, xrounds = rmax[0], rmax[1]

        sm_me = lax.dynamic_slice_in_dim(jnp.where(pres > 0, smap, -1), me * per, per, 0).reshape(vs)

        def gather_round(r, wait_for=None):
            hit = lax.broadcasted_iota(i32, (ROWS, vs), 0) == (sm_me - r * ROWS)[None, :]
            rows = jnp.sum(jnp.where(hit, lax.broadcasted_iota(i32, (ROWS, vs), 1), 0), axis=1)
            x0 = jnp.take(E, rows, axis=0, mode="clip")
            x1, x2 = send(x0, right), send(x0, left)
            x3 = [send(x1[:ROWS // 2], right), send(x2[ROWS // 2:], left)]
            lane = jnp.concatenate([x0, x1, x2] + x3, axis=0)
            xt = jnp.concatenate([lane, send(lane, twin)], axis=0)
            if wait_for is not None:
                xt = tie(xt, wait_for)
            xf = xt.astype(f32)
            rs = lax.rsqrt(jnp.mean(xf * xf, axis=-1, keepdims=True) + EPS)
            ntab = ((xf * rs) * gf).astype(bf16)
            key = slot - r * ROWS
            tix = jnp.where((key >= 0) & (key < ROWS), place * ROWS + key, -1)
            oht = (tix[:, None] == lax.broadcasted_iota(i32, (nt, ntp * ROWS), 1)).astype(bf16)
            n = mm(oht, ntab)
            tih = lax.dynamic_slice_in_dim(tix.reshape(nk, t), me * ts, ts, 1).reshape(-1)
            ohh = (tih[:, None] == lax.broadcasted_iota(i32, (nl, ntp * ROWS), 1)).astype(bf16)
            return n, dot(ohh, xt).astype(bf16)

        def more(c):
            r, n, xl = c
            n2, xl2 = gather_round(r)
            return r + 1, n + n2, xl + xl2

        n, xl = gather_round(0, last)
        _, n, xl = lax.while_loop(lambda c: c[0] < rounds, more, (i32(1), n, xl))

        for c in range(1, nc):
            after(c, n)
            pass_on(c, ch)
        u = mm(n, W)
        for c in range(nc):
            after(c, (relay[c], u))
        dns = []
        for c in range(nc):
            kc, ka = sizes[c], sizes[c] // 2
            dns.append(term(c, ch, 0, ka) + relay[c][0] + near[c][1][:ka])
            dns.append(term(c, ch, ka, kc) + near[c][0][ka:] + relay[c][1])
        dn = jnp.concatenate(dns, axis=0).reshape(nl, d)

        xf = xl.astype(f32)
        rs = lax.rsqrt(jnp.mean(xf * xf, axis=-1, keepdims=True) + EPS)
        nh = xf * rs
        gdn = gf * dn
        dx = dres.reshape(nl, d).astype(f32) + rs * (gdn - nh * jnp.mean(nh * gdn, axis=-1, keepdims=True))
        dxb = dx.astype(bf16)
        dgp = jnp.sum(dn * nh, axis=0)

        ownm = lax.dynamic_index_in_dim(ownh, me, 0, keepdims=False)
        rankm = lax.dynamic_index_in_dim(rank, me, 0, keepdims=False)

        def send_round(r):
            key = rankm - r * CAP
            q = jnp.where((key >= 0) & (key < CAP), ownm * CAP + key, -1)
            oh = (lax.broadcasted_iota(i32, (ntp * CAP, nl), 0) == q[None, :]).astype(bf16)
            b = dot(oh, dxb).astype(bf16)
            got = lax.all_to_all(b.reshape(ntp, CAP, d), "tp", 0, 0, tiled=True).reshape(ntp * CAP, d)
            sends.append((b, got))
            hit = (ownh == me)[:, None, :] & ((rank - r * CAP)[:, None, :] == lax.broadcasted_iota(i32, (ntp, CAP, nl), 1))
            rows = (jnp.sum(jnp.where(hit, (idh - lo + 1)[:, None, :], 0), axis=2) - 1).reshape(-1)
            ohr = (lax.broadcasted_iota(i32, (vs, ntp * CAP), 0) == rows[None, :]).astype(bf16)
            return dot(ohr, got)

        sends = []
        dE = send_round(0)
        dW = dot(n, du.reshape(nt, fs), c0)
        dgp = tie(dgp, sends[0][1])
        dg = jnp.sum(lax.all_to_all(jnp.broadcast_to(dgp, (ntp, d)), "tp", 0, 0, tiled=True), axis=0)
        _, dE = lax.while_loop(lambda c: c[0] < xrounds, lambda c: (c[0] + 1, c[1] + send_round(c[0])), (i32(1), dE))
        return u.reshape(nk, t, fs), xl.reshape(nk, ts, d), dE, dW, dg


    return jax.shard_map(
        work,
        mesh=mesh,
        in_specs=(P("dp", None), P("tp", None), P(None), P(None, "tp"), P("dp", None, "tp"), P("dp", "tp", None)),
        out_specs=(P("dp", None, "tp"), P("dp", "tp", None), P(("dp", "tp"), None), P("dp", "tp"), P("dp")),
        check_vma=False,
    )
```

```python
import jax
import jax.numpy as jnp
from jax import lax
from jax.experimental import pallas as pl
from jax.experimental.pallas import tpu as pltpu
from jax.sharding import PartitionSpec as P


EPS = 1e-6
ROWS = 176
CAP = 96
LANES = 128


def terms_kernel(co, a_ref, w_ref, keep_ref, give_ref):
    m, t, fs = a_ref.shape
    nch, _, ts, tn = keep_ref.shape
    r = lax.dot_general(a_ref[...].reshape(m * t, fs), w_ref[...], (((1,), (1,)), ((), ())), preferred_element_type=jnp.float32)
    r = r.astype(jnp.bfloat16).reshape(m, nch, 2, ts, tn)
    north = co[0] == 1
    for chip in range(nch):
        keep_ref[chip] = jnp.where(north, r[:, chip, 1], r[:, chip, 0])
        give_ref[chip] = jnp.where(north, r[:, chip, 0], r[:, chip, 1])


def spread_kernel(ch, ar, br, al, bl, r_ref, l_ref):
    f32 = jnp.float32
    r_ref[...] = ar[0].astype(f32) + br[0].astype(f32)
    l_ref[...] = al[0].astype(f32) + bl[0].astype(f32)


def lane_kernel(x0, x1, x2, x3, x4, o_ref):
    at = 0
    for x in (x0, x1, x2, x3, x4):
        o_ref[at:at + x.shape[0], :] = x[...]
        at += x.shape[0]


def solution(mesh):
    ntp = mesh.shape["tp"]
    nch = ntp // 2
    f32, bf16, i32 = jnp.float32, jnp.bfloat16, jnp.int32
    c0 = (((0,), (0,)), ((), ()))
    right = [(i, (i + 2) % ntp) for i in range(ntp)]
    left = [(i, (i - 2) % ntp) for i in range(ntp)]
    twin = [(i, i ^ 1) for i in range(ntp)]

    def dot(a, b, dims=(((1,), (0,)), ((), ()))):
        return lax.dot_general(a, b, dims, preferred_element_type=f32)

    def send(a, ring, axis="tp"):
        return lax.ppermute(a, axis, ring)

    def mm(*a):
        return dot(*a).astype(bf16)

    def tie(a, b):
        return lax.optimization_barrier((a, b))[0]

    def work(ids, E, g, W, du, dres):
        vs, d = E.shape
        nk, t = ids.shape
        ts = t // ntp
        fs = W.shape[1]
        nt = nk * t
        nl = nk * ts
        me = lax.axis_index("tp")
        ch, co = me // 2, me % 2
        lo = me * vs
        gf = g.astype(f32)

        sizes = (nk // 2, nk // 2)
        starts = (0, nk // 2)
        nc = len(sizes)

        def pick1(a, chip, k0, k1):
            return lax.dynamic_slice(a, (chip % nch, k0, 0, 0), (1, k1 - k0, ts, d)).reshape(k1 - k0, ts, d).astype(f32)

        ps, gots, near = [], [], []

        def term(c, chip, k0, k1):
            return pick1(ps[c], chip, k0, k1) + pick1(gots[c], chip, k0, k1)

        def after(c, x):
            ps[c], gots[c], _ = lax.optimization_barrier((ps[c], gots[c], x))

        def spread(c):
            kc = sizes[c]
            kb = 2
            na = kc // 2 // kb
            part = (1, kb, ts, d)

            def at(a, b):
                return pl.BlockSpec(part, lambda k, s: (lax.rem(s[0] + jnp.where(k < na, a, b), nch), k, 0, 0))

            rs, ls = at(2, 1), at(nch - 1, 2)
            out = pl.BlockSpec((kb, ts, d), lambda k, s: (k, 0, 0))
            to_r, to_l = pl.pallas_call(
                spread_kernel,
                grid_spec=pltpu.PrefetchScalarGridSpec(num_scalar_prefetch=1, grid=(kc // kb,), in_specs=[rs, rs, ls, ls], out_specs=[out, out]),
                out_shape=[jax.ShapeDtypeStruct((kc, ts, d), f32)] * 2,
                cost_estimate=pl.CostEstimate(flops=20 * kc * ts * d, bytes_accessed=16 * kc * ts * d, transcendentals=0),
            )(ch.reshape(1), ps[c], gots[c], ps[c], gots[c])
            near.append((send(to_r, right), send(to_l, left)))
            return to_l

        for c in range(nc):
            kc = sizes[c]
            half = jax.ShapeDtypeStruct((nch, kc, ts, d), bf16)
            kb, tn = kc, d // 6
            k0 = starts[c]
            out = pl.BlockSpec((nch, kb, ts, tn), lambda i, j, s: (0, i, 0, j))
            keep, give = pl.pallas_call(
                terms_kernel,
                grid_spec=pltpu.PrefetchScalarGridSpec(
                    num_scalar_prefetch=1,
                    grid=(kc // kb, d // tn),
                    in_specs=[
                        pl.BlockSpec((pl.Element(kb), pl.Element(t), pl.Element(fs)), lambda i, j, s, k0=k0: (k0, 0, 0)),
                        pl.BlockSpec((tn, fs), lambda i, j, s: (j, 0)),
                    ],
                    out_specs=[out, out],
                ),
                out_shape=[half, half],
                compiler_params=pltpu.CompilerParams(vmem_limit_bytes=48 * 1024 * 1024),
                cost_estimate=pl.CostEstimate(flops=2 * kc * t * d * fs, bytes_accessed=4 * kc * t * d, transcendentals=0),
            )(co.reshape(1), du, W)
            ps.append(keep)
            gots.append(send(give, twin))
        for c in range(nc):
            last = spread(c)

        relay = []

        def pass_on(c, chip):
            kc, ka = sizes[c], sizes[c] // 2
            qa = term(c, chip + 1, 0, ka) + near[c][0][:ka]
            qb = term(c, chip + nch - 1, ka, kc) + near[c][1][ka:]
            relay.append((send(qa, right), send(qb, left)))

        after(0, last)
        pass_on(0, ch)

        idf = ids.reshape(-1)
        nhi = ntp * vs // LANES
        per = vs // LANES
        ohi = (idf[:, None] // LANES == lax.broadcasted_iota(i32, (nt, nhi), 1)).astype(bf16)
        olo = (idf[:, None] % LANES == lax.broadcasted_iota(i32, (nt, LANES), 1)).astype(bf16)
        pres = (dot(ohi, olo, c0) > 0).astype(bf16)
        r0 = lax.broadcasted_iota(i32, (LANES, LANES), 0)
        r1 = lax.broadcasted_iota(i32, (LANES, LANES), 1)
        within = dot(pres, (r0 < r1).astype(bf16))
        h0 = lax.broadcasted_iota(i32, (nhi, nhi), 0)
        h1 = lax.broadcasted_iota(i32, (nhi, nhi), 1)
        above = dot(((h1 < h0) & (h0 // per == h1 // per)).astype(bf16), jnp.sum(pres.astype(f32), axis=1, keepdims=True).astype(bf16))
        smap = (within + above).astype(i32)
        s_hi, s_lo = (smap // LANES).astype(bf16), (smap % LANES).astype(bf16)
        slot = jnp.sum((dot(ohi, s_hi) * LANES + dot(ohi, s_lo)) * olo.astype(f32), axis=1).astype(i32)
        own = idf // vs
        away = (own // 2 + nch - ch) % nch
        place = jnp.where(own % 2 == co, 0, nch) + jnp.where(away == 0, 0, jnp.where(away == nch - 1, 1, away + 1))
        idh = ids.reshape(nk, ntp, ts).transpose(1, 0, 2).reshape(ntp, nl)
        ownh = idh // vs
        oc = (ownh[:, None, :] == lax.broadcasted_iota(i32, (ntp, ntp, nl), 1)).astype(bf16).reshape(ntp * ntp, nl)
        j0 = lax.broadcasted_iota(i32, (nl, nl), 0)
        j1 = lax.broadcasted_iota(i32, (nl, nl), 1)
        before = dot(oc, (j0 < j1).astype(bf16))
        rank = jnp.sum((before * oc.astype(f32)).reshape(ntp, ntp, nl), axis=1).astype(i32)

        rmax = jnp.stack([jnp.max(slot) // ROWS, jnp.max(rank) // CAP]) + 1
        step = 1
        while step < mesh.shape["dp"]:
            ring = [(i, (i + step) % mesh.shape["dp"]) for i in range(mesh.shape["dp"])]
            rmax = jnp.maximum(rmax, send(rmax, ring, "dp"))
            step *= 2
        rounds, xrounds = rmax[0], rmax[1]

        sm_me = lax.dynamic_slice_in_dim(jnp.where(pres > 0, smap, -1), me * per, per, 0).reshape(vs)

        def gather_round(r, wait_for=None):
            hit = lax.broadcasted_iota(i32, (ROWS, vs), 0) == (sm_me - r * ROWS)[None, :]
            rows = jnp.sum(jnp.where(hit, lax.broadcasted_iota(i32, (ROWS, vs), 1), 0), axis=1)
            x0 = jnp.take(E, rows, axis=0, mode="clip")
            x1, x2 = send(x0, right), send(x0, left)
            x3 = [send(x1[:ROWS // 2], right), send(x2[ROWS // 2:], left)]
            lane = pl.pallas_call(
                lane_kernel,
                out_shape=jax.ShapeDtypeStruct((nch * ROWS, d), bf16),
                cost_estimate=pl.CostEstimate(flops=20 * nch * ROWS * d, bytes_accessed=4 * nch * ROWS * d, transcendentals=0),
            )(x0, x1, x2, *x3)
            xt = jnp.concatenate([lane, send(lane, twin)], axis=0)
            if wait_for is not None:
                xt = tie(xt, wait_for)
            xf = xt.astype(f32)
            rs = lax.rsqrt(jnp.mean(xf * xf, axis=-1, keepdims=True) + EPS)
            ntab = ((xf * rs) * gf).astype(bf16)
            key = slot - r * ROWS
            tix = jnp.where((key >= 0) & (key < ROWS), place * ROWS + key, -1)
            oht = (tix[:, None] == lax.broadcasted_iota(i32, (nt, ntp * ROWS), 1)).astype(bf16)
            n = mm(oht, ntab)
            tih = lax.dynamic_slice_in_dim(tix.reshape(nk, t), me * ts, ts, 1).reshape(-1)
            ohh = (tih[:, None] == lax.broadcasted_iota(i32, (nl, ntp * ROWS), 1)).astype(bf16)
            return n, mm(ohh, xt)

        def more(c):
            r, n, xl = c
            n2, xl2 = gather_round(r)
            return r + 1, n + n2, xl + xl2

        n, xl = gather_round(0, last)
        _, n, xl = lax.while_loop(lambda c: c[0] < rounds, more, (i32(1), n, xl))

        for c in range(1, nc):
            after(c, n)
            pass_on(c, ch)
        u = mm(n, W)
        for c in range(nc):
            after(c, (relay[c], u))
        dns = []
        for c in range(nc):
            kc, ka = sizes[c], sizes[c] // 2
            dns.append(term(c, ch, 0, ka) + relay[c][0] + near[c][1][:ka])
            dns.append(term(c, ch, ka, kc) + near[c][0][ka:] + relay[c][1])
        dn = jnp.concatenate(dns, axis=0).reshape(nl, d)

        xf = xl.astype(f32)
        rs = lax.rsqrt(jnp.mean(xf * xf, axis=-1, keepdims=True) + EPS)
        nh = xf * rs
        gdn = gf * dn
        dx = dres.reshape(nl, d).astype(f32) + rs * (gdn - nh * jnp.mean(nh * gdn, axis=-1, keepdims=True))
        dxb = dx.astype(bf16)
        dgp = jnp.sum(dn * nh, axis=0)

        ownm = lax.dynamic_index_in_dim(ownh, me, 0, keepdims=False)
        rankm = lax.dynamic_index_in_dim(rank, me, 0, keepdims=False)

        def send_round(r):
            key = rankm - r * CAP
            q = jnp.where((key >= 0) & (key < CAP), ownm * CAP + key, -1)
            oh = (lax.broadcasted_iota(i32, (ntp * CAP, nl), 0) == q[None, :]).astype(bf16)
            b = dot(oh, dxb).astype(bf16)
            got = lax.all_to_all(b.reshape(ntp, CAP, d), "tp", 0, 0, tiled=True).reshape(ntp * CAP, d)
            sends.append((b, got))
            hit = (ownh == me)[:, None, :] & ((rank - r * CAP)[:, None, :] == lax.broadcasted_iota(i32, (ntp, CAP, nl), 1))
            rows = (jnp.sum(jnp.where(hit, (idh - lo + 1)[:, None, :], 0), axis=2) - 1).reshape(-1)
            ohr = (lax.broadcasted_iota(i32, (vs, ntp * CAP), 0) == rows[None, :]).astype(bf16)
            return dot(ohr, got)

        sends = []
        dE = send_round(0)
        dW = dot(n, du.reshape(nt, fs), c0)
        dgp = tie(dgp, sends[0][1])
        dg = jnp.sum(lax.all_to_all(jnp.broadcast_to(dgp, (ntp, d)), "tp", 0, 0, tiled=True), axis=0)
        _, dE = lax.while_loop(lambda c: c[0] < xrounds, lambda c: (c[0] + 1, c[1] + send_round(c[0])), (i32(1), dE))
        return u.reshape(nk, t, fs), xl.reshape(nk, ts, d), dE, dW, dg


    return jax.shard_map(
        work,
        mesh=mesh,
        in_specs=(P("dp", None), P("tp", None), P(None), P(None, "tp"), P("dp", None, "tp"), P("dp", "tp", None)),
        out_specs=(P("dp", None, "tp"), P("dp", "tp", None), P(("dp", "tp"), None), P("dp", "tp"), P("dp")),
        check_vma=False,
    )
```

```python
import jax
import jax.numpy as jnp
from jax import lax
from jax.experimental import pallas as pl
from jax.experimental.pallas import tpu as pltpu
from jax.sharding import PartitionSpec as P


EPS = 1e-6
ROWS = 176
CAP = 96
LANES = 128


def terms_kernel(co, a_ref, w_ref, keep_ref, give_ref):
    m, t, fs = a_ref.shape
    nch, _, ts, tn = keep_ref.shape
    r = lax.dot_general(a_ref[...].reshape(m * t, fs), w_ref[...], (((1,), (1,)), ((), ())), preferred_element_type=jnp.float32)
    r = r.astype(jnp.bfloat16).reshape(m, nch, 2, ts, tn)
    north = co[0] == 1
    for chip in range(nch):
        keep_ref[chip] = jnp.where(north, r[:, chip, 1], r[:, chip, 0])
        give_ref[chip] = jnp.where(north, r[:, chip, 0], r[:, chip, 1])


def spread_kernel(ch, ar, br, al, bl, r_ref, l_ref):
    f32 = jnp.float32
    r_ref[...] = ar[0].astype(f32) + br[0].astype(f32)
    l_ref[...] = al[0].astype(f32) + bl[0].astype(f32)


def lane_kernel(x0, x1, x2, x3, x4, o_ref):
    at = 0
    for x in (x0, x1, x2, x3, x4):
        o_ref[at:at + x.shape[0], :] = x[...]
        at += x.shape[0]


def dx_kernel(ch, keep, got, ra, la, rb, lb, x_ref, dres, g_ref, *rest):
    dx_ref, dg_ref = rest[-2:]
    f32 = jnp.float32
    k = pl.program_id(0)
    far = jnp.where(k < pl.num_programs(0) // 2, ra[...] + la[...], rb[...] + lb[...])
    dn = keep[0].astype(f32) + got[0].astype(f32) + far
    x = x_ref[...].astype(f32)
    rs = lax.rsqrt(jnp.mean(x * x, axis=-1, keepdims=True) + EPS)
    nh = x * rs
    gdn = g_ref[...] * dn
    dx = dres[...].astype(f32) + rs * (gdn - nh * jnp.mean(nh * gdn, axis=-1, keepdims=True))
    dx_ref[...] = dx.astype(jnp.bfloat16)

    @pl.when(k == 0)
    def _():
        dg_ref[...] = jnp.zeros_like(dg_ref)

    dg_ref[...] += jnp.sum(jnp.sum(dn * nh, axis=0), axis=0, keepdims=True)


def solution(mesh):
    ntp = mesh.shape["tp"]
    nch = ntp // 2
    f32, bf16, i32 = jnp.float32, jnp.bfloat16, jnp.int32
    c0 = (((0,), (0,)), ((), ()))
    right = [(i, (i + 2) % ntp) for i in range(ntp)]
    left = [(i, (i - 2) % ntp) for i in range(ntp)]
    twin = [(i, i ^ 1) for i in range(ntp)]

    def dot(a, b, dims=(((1,), (0,)), ((), ()))):
        return lax.dot_general(a, b, dims, preferred_element_type=f32)

    def send(a, ring, axis="tp"):
        return lax.ppermute(a, axis, ring)

    def mm(*a):
        return dot(*a).astype(bf16)

    def tie(a, b):
        return lax.optimization_barrier((a, b))[0]

    def work(ids, E, g, W, du, dres):
        vs, d = E.shape
        nk, t = ids.shape
        ts = t // ntp
        fs = W.shape[1]
        nt = nk * t
        nl = nk * ts
        me = lax.axis_index("tp")
        ch, co = me // 2, me % 2
        lo = me * vs
        gf = g.astype(f32)

        sizes = (nk // 2, nk // 2)
        starts = (0, nk // 2)
        nc = len(sizes)

        def pick1(a, chip, k0, k1):
            return lax.dynamic_slice(a, (chip % nch, k0, 0, 0), (1, k1 - k0, ts, d)).reshape(k1 - k0, ts, d).astype(f32)

        ps, gots, near = [], [], []

        def term(c, chip, k0, k1):
            return pick1(ps[c], chip, k0, k1) + pick1(gots[c], chip, k0, k1)

        def after(c, x):
            ps[c], gots[c], _ = lax.optimization_barrier((ps[c], gots[c], x))

        def spread(c):
            kc = sizes[c]
            kb = 2
            na = kc // 2 // kb
            part = (1, kb, ts, d)

            def at(a, b):
                return pl.BlockSpec(part, lambda k, s: (lax.rem(s[0] + jnp.where(k < na, a, b), nch), k, 0, 0))

            rs, ls = at(2, 1), at(nch - 1, 2)
            out = pl.BlockSpec((kb, ts, d), lambda k, s: (k, 0, 0))
            to_r, to_l = pl.pallas_call(
                spread_kernel,
                grid_spec=pltpu.PrefetchScalarGridSpec(num_scalar_prefetch=1, grid=(kc // kb,), in_specs=[rs, rs, ls, ls], out_specs=[out, out]),
                out_shape=[jax.ShapeDtypeStruct((kc, ts, d), f32)] * 2,
                cost_estimate=pl.CostEstimate(flops=20 * kc * ts * d, bytes_accessed=16 * kc * ts * d, transcendentals=0),
            )(ch.reshape(1), ps[c], gots[c], ps[c], gots[c])
            near.append((send(to_r, right), send(to_l, left)))
            return to_l

        for c in range(nc):
            kc = sizes[c]
            half = jax.ShapeDtypeStruct((nch, kc, ts, d), bf16)
            kb, tn = kc, d // 6
            k0 = starts[c]
            out = pl.BlockSpec((nch, kb, ts, tn), lambda i, j, s: (0, i, 0, j))
            keep, give = pl.pallas_call(
                terms_kernel,
                grid_spec=pltpu.PrefetchScalarGridSpec(
                    num_scalar_prefetch=1,
                    grid=(kc // kb, d // tn),
                    in_specs=[
                        pl.BlockSpec((pl.Element(kb), pl.Element(t), pl.Element(fs)), lambda i, j, s, k0=k0: (k0, 0, 0)),
                        pl.BlockSpec((tn, fs), lambda i, j, s: (j, 0)),
                    ],
                    out_specs=[out, out],
                ),
                out_shape=[half, half],
                compiler_params=pltpu.CompilerParams(vmem_limit_bytes=48 * 1024 * 1024),
                cost_estimate=pl.CostEstimate(flops=2 * kc * t * d * fs, bytes_accessed=4 * kc * t * d, transcendentals=0),
            )(co.reshape(1), du, W)
            ps.append(keep)
            gots.append(send(give, twin))
        for c in range(nc):
            last = spread(c)

        relay = []

        def pass_on(c, chip):
            kc, ka = sizes[c], sizes[c] // 2
            qa = term(c, chip + 1, 0, ka) + near[c][0][:ka]
            qb = term(c, chip + nch - 1, ka, kc) + near[c][1][ka:]
            relay.append((send(qa, right), send(qb, left)))

        after(0, last)
        pass_on(0, ch)

        idf = ids.reshape(-1)
        nhi = ntp * vs // LANES
        per = vs // LANES
        ohi = (idf[:, None] // LANES == lax.broadcasted_iota(i32, (nt, nhi), 1)).astype(bf16)
        olo = (idf[:, None] % LANES == lax.broadcasted_iota(i32, (nt, LANES), 1)).astype(bf16)
        pres = (dot(ohi, olo, c0) > 0).astype(bf16)
        r0 = lax.broadcasted_iota(i32, (LANES, LANES), 0)
        r1 = lax.broadcasted_iota(i32, (LANES, LANES), 1)
        within = dot(pres, (r0 < r1).astype(bf16))
        h0 = lax.broadcasted_iota(i32, (nhi, nhi), 0)
        h1 = lax.broadcasted_iota(i32, (nhi, nhi), 1)
        above = dot(((h1 < h0) & (h0 // per == h1 // per)).astype(bf16), jnp.sum(pres.astype(f32), axis=1, keepdims=True).astype(bf16))
        smap = (within + above).astype(i32)
        s_hi, s_lo = (smap // LANES).astype(bf16), (smap % LANES).astype(bf16)
        slot = jnp.sum((dot(ohi, s_hi) * LANES + dot(ohi, s_lo)) * olo.astype(f32), axis=1).astype(i32)
        own = idf // vs
        away = (own // 2 + nch - ch) % nch
        place = jnp.where(own % 2 == co, 0, nch) + jnp.where(away == 0, 0, jnp.where(away == nch - 1, 1, away + 1))
        idh = ids.reshape(nk, ntp, ts).transpose(1, 0, 2).reshape(ntp, nl)
        ownh = idh // vs
        oc = (ownh[:, None, :] == lax.broadcasted_iota(i32, (ntp, ntp, nl), 1)).astype(bf16).reshape(ntp * ntp, nl)
        j0 = lax.broadcasted_iota(i32, (nl, nl), 0)
        j1 = lax.broadcasted_iota(i32, (nl, nl), 1)
        before = dot(oc, (j0 < j1).astype(bf16))
        rank = jnp.sum((before * oc.astype(f32)).reshape(ntp, ntp, nl), axis=1).astype(i32)

        rmax = jnp.stack([jnp.max(slot) // ROWS, jnp.max(rank) // CAP]) + 1
        step = 1
        while step < mesh.shape["dp"]:
            ring = [(i, (i + step) % mesh.shape["dp"]) for i in range(mesh.shape["dp"])]
            rmax = jnp.maximum(rmax, send(rmax, ring, "dp"))
            step *= 2
        rounds, xrounds = rmax[0], rmax[1]

        sm_me = lax.dynamic_slice_in_dim(jnp.where(pres > 0, smap, -1), me * per, per, 0).reshape(vs)

        def gather_round(r, wait_for=None):
            hit = lax.broadcasted_iota(i32, (ROWS, vs), 0) == (sm_me - r * ROWS)[None, :]
            rows = jnp.sum(jnp.where(hit, lax.broadcasted_iota(i32, (ROWS, vs), 1), 0), axis=1)
            x0 = jnp.take(E, rows, axis=0, mode="clip")
            x1, x2 = send(x0, right), send(x0, left)
            x3 = [send(x1[:ROWS // 2], right), send(x2[ROWS // 2:], left)]
            lane = pl.pallas_call(
                lane_kernel,
                out_shape=jax.ShapeDtypeStruct((nch * ROWS, d), bf16),
                cost_estimate=pl.CostEstimate(flops=20 * nch * ROWS * d, bytes_accessed=4 * nch * ROWS * d, transcendentals=0),
            )(x0, x1, x2, *x3)
            xt = jnp.concatenate([lane, send(lane, twin)], axis=0)
            if wait_for is not None:
                xt = tie(xt, wait_for)
            xf = xt.astype(f32)
            rs = lax.rsqrt(jnp.mean(xf * xf, axis=-1, keepdims=True) + EPS)
            ntab = ((xf * rs) * gf).astype(bf16)
            key = slot - r * ROWS
            tix = jnp.where((key >= 0) & (key < ROWS), place * ROWS + key, -1)
            oht = (tix[:, None] == lax.broadcasted_iota(i32, (nt, ntp * ROWS), 1)).astype(bf16)
            n = mm(oht, ntab)
            tih = lax.dynamic_slice_in_dim(tix.reshape(nk, t), me * ts, ts, 1).reshape(-1)
            ohh = (tih[:, None] == lax.broadcasted_iota(i32, (nl, ntp * ROWS), 1)).astype(bf16)
            return n, mm(ohh, xt)

        def more(c):
            r, n, xl = c
            n2, xl2 = gather_round(r)
            return r + 1, n + n2, xl + xl2

        n, xl = gather_round(0, last)
        _, n, xl = lax.while_loop(lambda c: c[0] < rounds, more, (i32(1), n, xl))

        for c in range(1, nc):
            after(c, n)
            pass_on(c, ch)
        u = mm(n, W)
        dxb, dgs = None, []
        for c in range(nc):
            after(c, (relay[c], u))
            kc, kb = sizes[c], 1
            na = kc // 2 // kb
            k0 = starts[c] // kb
            part = (kb, ts, d)
            mine = pl.BlockSpec((1,) + part, lambda k, s: (s[0], k, 0, 0))
            low = pl.BlockSpec(part, lambda k, s, na=na: (jnp.minimum(k, na - 1), 0, 0))
            high = pl.BlockSpec(part, lambda k, s, na=na: (jnp.maximum(k, na), 0, 0))
            high0 = pl.BlockSpec(part, lambda k, s, na=na: (jnp.maximum(k - na, 0), 0, 0))
            tok = pl.BlockSpec(part, lambda k, s, k0=k0: (k0 + k, 0, 0))
            row = pl.BlockSpec((1, d), lambda k, s: (0, 0))
            ins = [ps[c], gots[c], relay[c][0], near[c][1], near[c][0], relay[c][1], xl.reshape(nk, ts, d), dres, gf.reshape(1, d)]
            specs = [mine, mine, low, low, high, high0, tok, tok, row]
            alias = {}
            if dxb is not None:
                ins.append(dxb)
                specs.append(pl.BlockSpec(memory_space=pl.ANY))
                alias = {len(ins): 0}
            dxb, dgc = pl.pallas_call(
                dx_kernel,
                grid_spec=pltpu.PrefetchScalarGridSpec(num_scalar_prefetch=1, grid=(kc // kb,), in_specs=specs, out_specs=[tok, row]),
                out_shape=[jax.ShapeDtypeStruct((nk, ts, d), bf16), jax.ShapeDtypeStruct((1, d), f32)],
                input_output_aliases=alias,
                compiler_params=pltpu.CompilerParams(vmem_limit_bytes=40 * 1024 * 1024),
                cost_estimate=pl.CostEstimate(flops=40 * kc * ts * d, bytes_accessed=18 * kc * ts * d, transcendentals=0),
            )(ch.reshape(1), *ins)
            dgs.append(dgc)
        dxb = dxb.reshape(nl, d)
        dgp = sum(dgs[1:], dgs[0])[0]

        ownm = lax.dynamic_index_in_dim(ownh, me, 0, keepdims=False)
        rankm = lax.dynamic_index_in_dim(rank, me, 0, keepdims=False)

        def send_round(r):
            key = rankm - r * CAP
            q = jnp.where((key >= 0) & (key < CAP), ownm * CAP + key, -1)
            oh = (lax.broadcasted_iota(i32, (ntp * CAP, nl), 0) == q[None, :]).astype(bf16)
            b = dot(oh, dxb).astype(bf16)
            got = lax.all_to_all(b.reshape(ntp, CAP, d), "tp", 0, 0, tiled=True).reshape(ntp * CAP, d)
            sends.append((b, got))
            hit = (ownh == me)[:, None, :] & ((rank - r * CAP)[:, None, :] == lax.broadcasted_iota(i32, (ntp, CAP, nl), 1))
            rows = (jnp.sum(jnp.where(hit, (idh - lo + 1)[:, None, :], 0), axis=2) - 1).reshape(-1)
            ohr = (lax.broadcasted_iota(i32, (vs, ntp * CAP), 0) == rows[None, :]).astype(bf16)
            return dot(ohr, got)

        sends = []
        dE = send_round(0)
        dW = dot(n, du.reshape(nt, fs), c0)
        dgp = tie(dgp, sends[0][1])
        dg = jnp.sum(lax.all_to_all(jnp.broadcast_to(dgp, (ntp, d)), "tp", 0, 0, tiled=True), axis=0)
        _, dE = lax.while_loop(lambda c: c[0] < xrounds, lambda c: (c[0] + 1, c[1] + send_round(c[0])), (i32(1), dE))
        return u.reshape(nk, t, fs), xl.reshape(nk, ts, d), dE, dW, dg


    return jax.shard_map(
        work,
        mesh=mesh,
        in_specs=(P("dp", None), P("tp", None), P(None), P(None, "tp"), P("dp", None, "tp"), P("dp", "tp", None)),
        out_specs=(P("dp", None, "tp"), P("dp", "tp", None), P(("dp", "tp"), None), P("dp", "tp"), P("dp")),
        check_vma=False,
    )
```
